32 devices in a mesh: section: 4 (over y, core), img: 8 (over z, x).
Axes of the slice: x: 2, y: 2, z: 4, core: 2. Of those that a mesh axis runs over, the one named last changes fastest.
Arguments:
- early_feats: bfloat16 [8, 4096, 1280], P('section', 'img'), may hold values from -6 to 6
- final_embed: bfloat16 [8, 4096, 256], P('section', 'img'), may hold values from -240 to 240
- prompt_counts: int32 [8], replicated, may hold values from 16 to 64, as said below
- box_pixels: int32 [8, 64, 4], replicated, may hold values from 0 to 1023
- pair_table: int32 [8], replicated, may hold values from 0 to 7, as said below
- token_table: float32 [8, 256], replicated, may hold values from -6 to 6
- pe_basis: float32 [2, 128], replicated, may hold values from -5 to 5
- w_early: bfloat16 [1280, 256], replicated, may hold values from -0.15625 to 0.15625
- attend_in: bfloat16 [2, 6, 256, 128], replicated, may hold values from -0.375 to 0.375
- attend_out: bfloat16 [2, 2, 128, 256], replicated, may hold values from -0.5 to 0.5
- mlp_up: bfloat16 [2, 256, 2048], replicated, may hold values from -0.375 to 0.375
- mlp_down: bfloat16 [2, 2048, 256], replicated, may hold values from -0.125 to 0.125
- w_hyper: bfloat16 [256, 256], replicated, may hold values from -0.375 to 0.375
Outputs:
- masks: float32 [8, 64, 4096], P('section', None, 'img')
The draws below stay inside these ranges and needn't reach their ends.
Inputs may be any that keep to these rules, and one draw needn't show every extreme that they name: `prompt_counts`: at least one image has all 64 prompts live. `pair_table`: a permutation of the images that maps all 2 images of an output group to the 2 images of one input group, in any order.
All inputs are finite; a program needn't handle non-finite values.
Results may differ from the reference program's by a relative error of at most 0.017.
The reference program's roundings to bfloat16 on the way count: a program that leaves them out, or rounds other values in their place, can miss the bound.
Values may be sent and summed in bfloat16 or wider, within the bound.
A program may use at most 64 MiB of HBM per device.

```python
import math
import jax
import jax.numpy as jnp
from jax import lax

D_EARLY = 1280
D = 256
DA = 128
HEADS = 8
MLP = 2048
GRID = 64
IMG_PIX = 1024
PROMPTS = 64
TOKS_P = 8
LAYERS = 2
IMGS = 2
POS = 4096
IMAGES = 8
N_SECTION = 4


def draw_final_embed(key, part):
    key_one, key_two = jax.random.split(jax.random.fold_in(key, 11))
    noise_vals = jnp.clip(jax.random.normal(key_one, (IMAGES, POS, D), jnp.float32), -6.0, 6.0)
    return noise_vals.astype(jnp.bfloat16)


def draw_prompt_counts(key, part):
    key_one, key_two = jax.random.split(jax.random.fold_in(key, 23))
    values = jax.random.randint(key_one, (IMAGES,), PROMPTS // 4, PROMPTS + 1, jnp.int32)
    fullest = jax.random.randint(key_two, (), 0, IMAGES, jnp.int32)
    return jnp.where(jnp.arange(IMAGES, dtype=jnp.int32) == fullest, PROMPTS, values).astype(jnp.int32)


def draw_pair_table(key, part):
    key_one, key_two = jax.random.split(jax.random.fold_in(key, 37))
    group_order = jax.random.permutation(key_one, N_SECTION).astype(jnp.int32)
    scores = jax.random.randint(key_two, (N_SECTION, IMGS), 0, 1 << 20, jnp.int32) * IMGS + jnp.arange(IMGS, dtype=jnp.int32)[None, :]
    inner = jnp.argsort(scores, axis=1).astype(jnp.int32)
    table = group_order[:, None] * IMGS + inner
    return table.reshape(IMAGES).astype(jnp.int32)


def place_ends(drawn, own_key, low, largest):
    extent = drawn.shape
    place = [jax.random.randint(jax.random.fold_in(own_key, axis), (), 0, extent[axis]) for axis in range(len(extent))]
    drawn = drawn.at[tuple(place)].set(low)
    longest = extent.index(max(extent))
    place[longest] = (place[longest] + 1) % extent[longest]
    return drawn.at[tuple(place)].set(largest)


def block_levels(own_key, dims, pieces, smallest, high):
    def one(axis_at, parts):
        draws = jax.random.uniform(jax.random.fold_in(jax.random.fold_in(own_key, 6), axis_at), (parts,), jnp.float32, smallest / len(pieces), high / len(pieces))
        return jnp.repeat(jnp.exp(draws), dims[axis_at] // parts).reshape((-1,) + (1,) * (len(dims) - axis_at - 1))

    level = one(*pieces[0])
    for cut in pieces[1:]:
        level = level * one(*cut)
    return level


def gaussian(rng, dims, scale, reach, cuts=(), held_as=jnp.bfloat16):
    values = scale * jax.random.normal(rng, dims, jnp.float32)
    if cuts:
        values = values * block_levels(rng, dims, cuts, -0.22, 0.18)
    return jnp.clip(values, -reach, reach).astype(held_as)


def setup_inputs(seed: int = 0) -> dict:
    arg_keys = jax.random.split(jax.random.key(seed), 14)
    return {
        "early_feats": gaussian(arg_keys[0], (IMAGES, POS, D_EARLY), 1.0, 6.0, ((0, 4), (1, 8))),
        "final_embed": draw_final_embed(jax.random.fold_in(arg_keys[13], 71), 0),
        "prompt_counts": draw_prompt_counts(jax.random.fold_in(arg_keys[13], 71), 0),
        "box_pixels": place_ends(jax.random.randint(arg_keys[3], (IMAGES, PROMPTS, 4), 0, IMG_PIX), jax.random.fold_in(arg_keys[3], 1), 0, IMG_PIX - 1).astype(jnp.int32),
        "pair_table": draw_pair_table(jax.random.fold_in(arg_keys[13], 71), 0),
        "token_table": gaussian(arg_keys[5], (TOKS_P, D), 1.0, 6.0, (), jnp.float32),
        "pe_basis": gaussian(arg_keys[6], (2, D // 2), 1.0, 5.0, (), jnp.float32),
        "w_early": gaussian(arg_keys[7], (D_EARLY, D), D_EARLY ** -0.5, 0.15625),
        "attend_in": gaussian(arg_keys[8], (LAYERS, 6, D, DA), D ** -0.5, 0.375),
        "attend_out": gaussian(arg_keys[9], (LAYERS, 2, DA, D), DA ** -0.5, 0.5),
        "mlp_up": gaussian(arg_keys[10], (LAYERS, D, MLP), D ** -0.5, 0.375),
        "mlp_down": gaussian(arg_keys[11], (LAYERS, MLP, D), MLP ** -0.5, 0.125),
        "w_hyper": gaussian(arg_keys[12], (D, D), D ** -0.5, 0.375),
    }


NORM_EPS = 0.01

def norm_rows(values):
    center = values - lax.optimization_barrier(jnp.mean(values, axis=-1, keepdims=True))
    spread = lax.optimization_barrier(jnp.mean(center * center, axis=-1, keepdims=True))
    return center / jnp.sqrt(spread + NORM_EPS)

def round_keep(values):
    return lax.optimization_barrier(values.astype(jnp.bfloat16)).astype(jnp.float32)

def fourier(coord_x, coord_y, pe_basis):
    phase = (2.0 * coord_x - 1.0)[..., None] * pe_basis[0] + (2.0 * coord_y - 1.0)[..., None] * pe_basis[1]
    phase = 2.0 * math.pi * phase
    return jnp.concatenate([jnp.sin(phase), jnp.cos(phase)], axis=-1)

def grid_code(index, pe_basis):
    column = (index % GRID).astype(jnp.float32)
    row_idx = (index // GRID).astype(jnp.float32)
    return fourier((column + 0.5) / GRID, (row_idx + 0.5) / GRID, pe_basis)

def start_tokens(box_rows, token_table, pe_basis):
    coords = (box_rows.astype(jnp.float32) + 0.5) / IMG_PIX
    corner_one = fourier(coords[:, 0], coords[:, 1], pe_basis)
    corner_two = fourier(coords[:, 2], coords[:, 3], pe_basis)
    slots = jnp.arange(TOKS_P)[None, :, None]
    tokens = token_table[None] + jnp.where(slots == TOKS_P - 2, corner_one[:, None, :], 0.0)
    tokens = tokens + jnp.where(slots == TOKS_P - 1, corner_two[:, None, :], 0.0)
    return tokens.reshape(-1, token_table.shape[-1])

def attend(queries, keys, values, live):
    query_rows = queries.shape[0]
    key_rows = keys.shape[0]
    head_size = queries.shape[1] // HEADS
    query_heads = queries.reshape(query_rows, HEADS, head_size).astype(jnp.float32)
    key_heads = keys.reshape(key_rows, HEADS, head_size).astype(jnp.float32)
    scores = jnp.einsum('qhd,khd->hqk', query_heads, key_heads) * head_size ** (-0.5)
    if live is not None:
        scores = jnp.where(live[None, None, :], scores, -jnp.inf)
    highest = lax.optimization_barrier(jnp.max(scores, axis=-1, keepdims=True))
    weights = round_keep(jnp.exp(scores - highest))
    value_heads = values.reshape(key_rows, HEADS, head_size).astype(jnp.float32)
    summed = jnp.einsum('hqk,khd->qhd', weights, value_heads)
    totals = lax.optimization_barrier(jnp.sum(weights, axis=-1))
    return (summed / jnp.transpose(totals)[:, :, None]).reshape(query_rows, HEADS * head_size)

def bdot(left, right):
    return jnp.dot(left, right, preferred_element_type=jnp.float32)

def decode(early_one, final_one, count_one, boxes_one, token_table, pe_basis, w_early, attend_in, attend_out, mlp_up, mlp_down, w_hyper):
    hq_part = round_keep(jax.nn.gelu(bdot(early_one, w_early), approximate=False))
    img_code = grid_code(jnp.arange(POS, dtype=jnp.int32), pe_basis)
    image = final_one.astype(jnp.float32)
    tokens = start_tokens(boxes_one, token_table, pe_basis)
    live_prompt = jnp.arange(PROMPTS, dtype=jnp.int32) < count_one
    live_token = jnp.repeat(live_prompt, TOKS_P)
    token_bf = tokens.astype(jnp.bfloat16)
    for layer in range(LAYERS):
        token_bf = tokens.astype(jnp.bfloat16)
        image_bf = image.astype(jnp.bfloat16)
        key_bf = (image + img_code).astype(jnp.bfloat16)
        query_one = bdot(token_bf, attend_in[layer, 0]).astype(jnp.bfloat16)
        keys_one = bdot(key_bf, attend_in[layer, 1]).astype(jnp.bfloat16)
        values_one = bdot(image_bf, attend_in[layer, 2]).astype(jnp.bfloat16)
        first_out = attend(query_one, keys_one, values_one, None)
        tok_two = norm_rows(tokens + bdot(first_out.astype(jnp.bfloat16), attend_out[layer, 0]))
        hidden = jax.nn.relu(bdot(tok_two.astype(jnp.bfloat16), mlp_up[layer])).astype(jnp.bfloat16)
        tok_three = norm_rows(tok_two + bdot(hidden, mlp_down[layer]))
        token_bf = tok_three.astype(jnp.bfloat16)
        query_two = bdot(key_bf, attend_in[layer, 3]).astype(jnp.bfloat16)
        keys_two = bdot(token_bf, attend_in[layer, 4]).astype(jnp.bfloat16)
        values_two = bdot(token_bf, attend_in[layer, 5]).astype(jnp.bfloat16)
        second_out = attend(query_two, keys_two, values_two, live_token)
        image = norm_rows(image + bdot(second_out.astype(jnp.bfloat16), attend_out[layer, 1]))
        tokens = tok_three
    hq_rows = token_bf.reshape(PROMPTS, TOKS_P, -1)[:, TOKS_P - 3]
    hyper = bdot(hq_rows, w_hyper).astype(jnp.bfloat16)
    mask_feats = (image + hq_part).astype(jnp.bfloat16)
    logits = bdot(hyper, jnp.transpose(mask_feats)) * D ** (-0.5)
    return jnp.where(live_prompt[:, None], logits, 0.0)

def reference(early_feats, final_embed, prompt_counts, box_pixels, pair_table, token_table, pe_basis, w_early, attend_in, attend_out, mlp_up, mlp_down, w_hyper):

    def one_image(index):
        picked = pair_table[index].astype(jnp.int32)
        return decode(early_feats[picked], final_embed[picked], prompt_counts[picked], box_pixels[picked], token_table, pe_basis, w_early, attend_in, attend_out, mlp_up, mlp_down, w_hyper)
    return lax.map(one_image, jnp.arange(IMAGES, dtype=jnp.int32))
```

```python
import math

import jax
import jax.numpy as jnp
from jax import lax
from jax.sharding import PartitionSpec as P

HEADS = 8
GRID = 64
IMG_PIX = 1024
TOKS_P = 8
LAYERS = 2


NORM_EPS = 0.01


def partner(x, axis, distance):
    return lax.ppermute(x, axis, [(i, i ^ 1 << distance) for i in range(lax.axis_size(axis))])


def shortened(x):
    return jax.tree.map(lambda a: a.astype(jnp.bfloat16) if a.dtype == jnp.float32 else a, x)


def norm_rows(values):
    center = values - jnp.mean(values, axis=-1, keepdims=True)
    spread = jnp.mean(center * center, axis=-1, keepdims=True)
    return center / jnp.sqrt(spread + NORM_EPS)


def fourier(coord_x, coord_y, pe_basis):
    phase = (2.0 * coord_x - 1.0)[..., None] * pe_basis[0] + (2.0 * coord_y - 1.0)[
        ..., None
    ] * pe_basis[1]
    phase = 2.0 * math.pi * phase
    return jnp.concatenate([jnp.sin(phase), jnp.cos(phase)], axis=-1)


def grid_code(index, pe_basis):
    column = (index % GRID).astype(jnp.float32)
    row_idx = (index // GRID).astype(jnp.float32)
    return fourier((column + 0.5) / GRID, (row_idx + 0.5) / GRID, pe_basis)


def start_tokens(box_rows, token_table, pe_basis):
    coords = (box_rows.astype(jnp.float32) + 0.5) / IMG_PIX
    corner_one = fourier(coords[:, 0], coords[:, 1], pe_basis)
    corner_two = fourier(coords[:, 2], coords[:, 3], pe_basis)
    slots = jnp.arange(TOKS_P)[None, :, None]
    tokens = token_table[None] + jnp.where(slots == TOKS_P - 2, corner_one[:, None, :], 0.0)
    tokens = tokens + jnp.where(slots == TOKS_P - 1, corner_two[:, None, :], 0.0)
    return tokens.reshape(-1, token_table.shape[-1])


def bdot(left, right):
    return jnp.dot(left, right, preferred_element_type=jnp.float32)


def make_hq(early_part, w_early):
    hq_part = jax.nn.gelu(bdot(early_part, w_early), approximate=False).astype(jnp.bfloat16)
    return lax.optimization_barrier(hq_part)


def shards(
    early_feats,
    final_embed,
    prompt_counts,
    box_pixels,
    pair_table,
    token_table,
    pe_basis,
    w_early,
    attend_in,
    attend_out,
    mlp_up,
    mlp_down,
    w_hyper,
):
    images = early_feats.shape[0]
    pos_dev = early_feats.shape[1]
    width = final_embed.shape[2]
    prompts = box_pixels.shape[1]
    devices = lax.axis_size("img")
    my_index = lax.axis_index("img")
    my_section = lax.axis_index("section")
    img_bits = images.bit_length() - 1
    all_bits = devices.bit_length() - 1
    my_bit = my_index & 1

    def split_images(part):
        pairs = part.reshape(part.shape[0] // 2, 2, part.shape[1], width)
        keep = lax.dynamic_index_in_dim(pairs, my_bit, 1, keepdims=False)
        send = lax.dynamic_index_in_dim(pairs, 1 - my_bit, 1, keepdims=False)
        got = partner(send, "img", 0)
        lower = jnp.where(my_bit == 0, keep, got)
        upper = jnp.where(my_bit == 0, got, keep)
        return jnp.concatenate([lower, upper], axis=1)

    final_here = split_images(final_embed)
    hq_here = split_images(make_hq(early_feats, w_early))
    held = 1
    held_pos = images * pos_dev
    members = devices // images
    my_rank = my_index // images
    table_offset = my_index % images
    first_pos = my_rank * held_pos
    mine = my_section * images + table_offset
    my_counts = lax.dynamic_slice_in_dim(prompt_counts, mine, held, 0)
    my_boxes = lax.dynamic_slice_in_dim(box_pixels, mine, held, 0)
    per_image = prompts * TOKS_P
    rows_all = held * per_image
    own_rows = rows_all // members
    head_size = attend_in.shape[-1] // HEADS
    scale = head_size ** (-0.5)
    tokens_start = start_tokens(my_boxes.reshape(-1, 4), token_table, pe_basis)
    tok_own = lax.dynamic_slice_in_dim(tokens_start, my_rank * own_rows, own_rows, 0)
    positions = first_pos + jnp.arange(held_pos, dtype=jnp.int32)
    img_code = grid_code(positions, pe_basis)
    image = final_here.astype(jnp.float32)
    live_prompt = jnp.arange(prompts, dtype=jnp.int32)[None, :] < my_counts[:, None]
    live_token = jnp.repeat(live_prompt, TOKS_P, axis=1)
    query_one = bdot(tokens_start.astype(jnp.bfloat16), attend_in[0, 0]).astype(jnp.bfloat16)
    hyper = None
    for layer in range(LAYERS):
        image_bf = image.astype(jnp.bfloat16)
        key_bf = (image + img_code[None]).astype(jnp.bfloat16)
        keys_one = bdot(key_bf, attend_in[layer, 1]).astype(jnp.bfloat16)
        values_one = bdot(image_bf, attend_in[layer, 2]).astype(jnp.bfloat16)
        query_heads = query_one.reshape(held, per_image, HEADS, head_size)
        key_heads = keys_one.reshape(held, held_pos, HEADS, head_size)
        value_heads = values_one.reshape(held, held_pos, HEADS, head_size)
        scores = (
            jnp.einsum(
                "iqhd,ikhd->ihqk", query_heads, key_heads, preferred_element_type=jnp.float32
            )
            * scale
        )
        values = jnp.max(scores, axis=-1)
        for peak_bit in range(img_bits, all_bits):
            values = jnp.maximum(values, partner(values, "img", peak_bit))
        weights = jnp.exp(scores - values[..., None]).astype(jnp.bfloat16)
        summed = jnp.einsum(
            "ihqk,ikhd->iqhd", weights, value_heads, preferred_element_type=jnp.float32
        ).reshape(rows_all, HEADS * head_size)
        totals = jnp.sum(weights.astype(jnp.float32), axis=-1)
        totals = jnp.transpose(totals, (0, 2, 1)).reshape(rows_all, HEADS)
        reduce_summed = summed
        reduce_totals = totals
        for reduce_bit in reversed(range(img_bits, all_bits)):
            reduce_my_bit = my_index >> reduce_bit & 1
            split_s = reduce_summed.reshape(2, reduce_summed.shape[0] // 2, reduce_summed.shape[1])
            split_t = reduce_totals.reshape(2, reduce_totals.shape[0] // 2, reduce_totals.shape[1])
            keep_s = lax.dynamic_index_in_dim(split_s, reduce_my_bit, 0, keepdims=False)
            keep_t = lax.dynamic_index_in_dim(split_t, reduce_my_bit, 0, keepdims=False)
            send_s = lax.dynamic_index_in_dim(split_s, 1 - reduce_my_bit, 0, keepdims=False)
            send_t = lax.dynamic_index_in_dim(split_t, 1 - reduce_my_bit, 0, keepdims=False)
            reduce_got = (
                partner(send_s.astype(jnp.bfloat16), "img", reduce_bit).astype(send_s.dtype),
                partner(send_t.astype(jnp.bfloat16), "img", reduce_bit).astype(send_t.dtype),
            )
            reduce_summed = keep_s + reduce_got[0]
            reduce_totals = keep_t + reduce_got[1]
        first_out = (
            reduce_summed.reshape(own_rows, HEADS, head_size) / reduce_totals[:, :, None]
        ).reshape(own_rows, HEADS * head_size)
        tok_two = norm_rows(tok_own + bdot(first_out.astype(jnp.bfloat16), attend_out[layer, 0]))
        hidden = jax.nn.relu(bdot(tok_two.astype(jnp.bfloat16), mlp_up[layer])).astype(jnp.bfloat16)
        tok_three = norm_rows(tok_two + bdot(hidden, mlp_down[layer]))
        three_own = tok_three.astype(jnp.bfloat16)
        last_layer = layer == LAYERS - 1
        rows = (three_own,)
        for collect_bit in range(img_bits, all_bits):
            collect_my_bit = my_index >> collect_bit & 1
            collect_got = jax.tree.map(
                lambda part, own: part.astype(own.dtype),
                partner(shortened(rows), "img", collect_bit),
                rows,
            )
            rows = tuple(
                (
                    jnp.concatenate(
                        [
                            jnp.where(collect_my_bit == 0, mine, theirs),
                            jnp.where(collect_my_bit == 0, theirs, mine),
                        ],
                        axis=0,
                    )
                    for mine, theirs in zip(rows, collect_got)
                )
            )
        three_all = rows[0]
        keys_two = bdot(three_all, attend_in[layer, 4]).astype(jnp.bfloat16)
        values_two = bdot(three_all, attend_in[layer, 5]).astype(jnp.bfloat16)
        if last_layer:
            hyper = bdot(three_all.reshape(-1, TOKS_P, width)[:, TOKS_P - 3], w_hyper).astype(
                jnp.bfloat16
            )
        else:
            query_one = bdot(three_all, attend_in[layer + 1, 0]).astype(jnp.bfloat16)
        query_two = (
            bdot(key_bf, attend_in[layer, 3])
            .astype(jnp.bfloat16)
            .reshape(held, held_pos, HEADS, head_size)
        )
        token_keys = keys_two.reshape(held, per_image, HEADS, head_size)
        token_values = values_two.reshape(held, per_image, HEADS, head_size)
        scores_two = (
            jnp.einsum("ikhd,iqhd->ihkq", query_two, token_keys, preferred_element_type=jnp.float32)
            * scale
        )
        scores_two = jnp.where(live_token[:, None, None, :], scores_two, -jnp.inf)
        highest_two = jnp.max(scores_two, axis=-1, keepdims=True)
        weights_two = jnp.exp(scores_two - highest_two).astype(jnp.bfloat16)
        summed_two = jnp.einsum(
            "ihkq,iqhd->ikhd", weights_two, token_values, preferred_element_type=jnp.float32
        )
        totals_two = jnp.transpose(jnp.sum(weights_two.astype(jnp.float32), axis=-1), (0, 2, 1))
        second_out = (summed_two / totals_two[..., None]).reshape(held, held_pos, HEADS * head_size)
        image = norm_rows(image + bdot(second_out.astype(jnp.bfloat16), attend_out[layer, 1]))
        tok_own = tok_three
    hyper_rows = hyper.reshape(held, prompts, width)
    mask_feats = (image + hq_here.astype(jnp.float32)).astype(jnp.bfloat16)
    logits = jnp.einsum(
        "ipc,ikc->ipk", hyper_rows, mask_feats, preferred_element_type=jnp.float32
    ) * width ** (-0.5)
    result = jnp.where(live_prompt[:, :, None], logits, 0.0).astype(jnp.bfloat16)
    for bit in reversed(range(img_bits)):
        my_bit = my_index >> bit & 1
        halves = result.reshape(result.shape[0], prompts, 2, result.shape[2] // 2)
        keep = lax.dynamic_index_in_dim(halves, my_bit, 2, keepdims=False)
        send = lax.dynamic_index_in_dim(halves, 1 - my_bit, 2, keepdims=False)
        got = partner(send, "img", bit)
        first = jnp.where(my_bit == 0, keep, got)
        second = jnp.where(my_bit == 0, got, keep)
        result = jnp.stack([first, second], axis=1).reshape(
            2 * keep.shape[0], prompts, keep.shape[2]
        )
    gathered = lax.all_gather(result, "section", axis=0, tiled=True)
    outputs = lax.dynamic_slice_in_dim(pair_table, my_section * images, images, 0)
    return jnp.concatenate(
        [
            lax.dynamic_slice_in_dim(gathered, outputs[i], 1, 0).astype(jnp.float32)
            for i in range(images)
        ]
    )


def solution(mesh):
    placed = (
        P("section", "img", None),
        P("section", "img", None),
        P(),
        P(),
        P(),
        P(),
        P(),
        P(),
        P(),
        P(),
        P(),
        P(),
        P(),
    )
    return jax.shard_map(
        shards, mesh=mesh, in_specs=placed, out_specs=P("section", None, "img"), check_vma=False
    )
```

```python
import functools
import math

import jax
import jax.numpy as jnp
from jax import lax
from jax.experimental import pallas as pl
from jax.experimental.pallas import tpu as pltpu
from jax.sharding import PartitionSpec as P

HEADS = 8
GRID = 64
IMG_PIX = 1024
TOKS_P = 8
LAYERS = 2


NORM_EPS = 0.01
MESH = pl.DeviceIdType.MESH


def norm_rows(values):
    center = values - jnp.mean(values, axis=-1, keepdims=True)
    spread = jnp.mean(center * center, axis=-1, keepdims=True)
    return center * lax.rsqrt(spread + NORM_EPS)


def fourier(coord_x, coord_y, pe_basis):
    phase = (2.0 * coord_x - 1.0)[..., None] * pe_basis[0] + (2.0 * coord_y - 1.0)[
        ..., None
    ] * pe_basis[1]
    phase = 2.0 * math.pi * phase
    return jnp.concatenate([jnp.sin(phase), jnp.cos(phase)], axis=-1)


def grid_code(first_pos, count, pe_basis):
    rows = count // GRID
    x = (jnp.arange(GRID, dtype=jnp.int32).astype(jnp.float32) + 0.5) / GRID
    y = ((first_pos // GRID + jnp.arange(rows, dtype=jnp.int32)).astype(jnp.float32) + 0.5) / GRID
    across = 2.0 * math.pi * ((2.0 * x - 1.0)[:, None] * pe_basis[0])[None]
    down = 2.0 * math.pi * ((2.0 * y - 1.0)[:, None] * pe_basis[1])[:, None]
    sin_a, cos_a, sin_d, cos_d = jnp.sin(across), jnp.cos(across), jnp.sin(down), jnp.cos(down)
    sines = sin_a * cos_d + cos_a * sin_d
    cosines = cos_a * cos_d - sin_a * sin_d
    return jnp.concatenate([sines, cosines], axis=-1).reshape(count, -1)


def start_tokens(box_rows, token_table, pe_basis):
    coords = (box_rows.astype(jnp.float32) + 0.5) / IMG_PIX
    corner_one = fourier(coords[:, 0], coords[:, 1], pe_basis)
    corner_two = fourier(coords[:, 2], coords[:, 3], pe_basis)
    slots = jnp.arange(TOKS_P)[None, :, None]
    tokens = token_table[None] + jnp.where(slots == TOKS_P - 2, corner_one[:, None, :], 0.0)
    tokens = tokens + jnp.where(slots == TOKS_P - 1, corner_two[:, None, :], 0.0)
    return tokens.reshape(-1, token_table.shape[-1])


def bdot(left, right):
    return jnp.dot(left, right, preferred_element_type=jnp.float32)


def make_hq(early_part, w_early):
    hq_part = jax.nn.gelu(bdot(early_part, w_early), approximate=False).astype(jnp.bfloat16)
    return lax.optimization_barrier(hq_part)


def tile_rows(rows, most):
    return min(rows, most)


def head_attend(queries, keys_ref, values_ref, key_rows, head_lanes, bias):
    total = None
    peaks = []
    for head in range(HEADS):
        picked = jnp.where(head_lanes == head, queries, jnp.zeros_like(queries))
        scores = lax.dot_general(
            picked, keys_ref[...], (((1,), (1,)), ((), ())), preferred_element_type=jnp.float32
        )
        if bias is not None:
            scores = scores + bias
        peak = jnp.max(scores, axis=-1, keepdims=True)
        weights = jnp.exp(scores - peak).astype(jnp.bfloat16)
        part = bdot(weights, values_ref[head, :key_rows])
        total = part if total is None else total + part
        peaks.append(peak)
    return total, peaks


def decode_kernel(
    members,
    final_ref,
    hq_ref,
    code_ref,
    tok0_ref,
    bias_ref,
    live_ref,
    win_ref,
    wout_ref,
    up_ref,
    down_ref,
    whyper_ref,
    out_ref,
    fin,
    hqs,
    img,
    tok,
    tok3b,
    vaug,
    q1,
    k1,
    q2,
    k2,
    part_a,
    part_l,
    lse,
    recv_a,
    recv_l,
    a1_all,
    swap_send,
    swap_recv,
    a_send,
    a_recv,
    l_send,
    l_recv,
    g_send,
    g_recv,
):
    me = lax.axis_index("img")
    bit = lax.rem(me, 2)
    rank = me // 2
    other = me + 1 - 2 * bit
    pos_dev = final_ref.shape[1]
    width = final_ref.shape[2]
    rows_all = tok.shape[0]
    own = rows_all // members
    held_pos = img.shape[0]
    inner = q1.shape[1]
    head_size = inner // HEADS
    scale = head_size ** (-0.5)

    def peer_rank(step):
        return lax.rem(rank + step, members)

    barrier = pltpu.get_barrier_semaphore()
    pl.semaphore_signal(barrier, inc=1, device_id={"img": other}, device_id_type=MESH)
    for step in range(1, members):
        pl.semaphore_signal(
            barrier, inc=1, device_id={"img": peer_rank(step) * 2 + bit}, device_id_type=MESH
        )
    pl.semaphore_wait(barrier, members)

    def send(src, dst, send_sem, recv_sem, target):
        copy = pltpu.make_async_remote_copy(
            src_ref=src,
            dst_ref=dst,
            send_sem=send_sem,
            recv_sem=recv_sem,
            device_id={"img": target},
            device_id_type=MESH,
        )
        copy.start()
        return copy

    swap_final = send(
        final_ref.at[1 - bit], fin.at[bit], swap_send.at[0], swap_recv.at[0], other
    )
    swap_hq = send(hq_ref.at[1 - bit], hqs.at[bit], swap_send.at[1], swap_recv.at[1], other)
    fin[bit] = final_ref[bit]
    hqs[bit] = hq_ref[bit]

    lane_head = lax.broadcasted_iota(jnp.int32, (1, inner), 1) // head_size
    lane = lax.broadcasted_iota(jnp.int32, (1, inner), 1)
    key_rows_max = vaug.shape[1]
    for head in range(HEADS):
        ones = jnp.where(lane_head == head, 1.0, 0.0)
        vaug[head, :, inner:] = jnp.broadcast_to(ones, (key_rows_max, inner)).astype(jnp.bfloat16)

    tok_tile = tile_rows(rows_all, 256)
    mlp_tile = tile_rows(rows_all, 256)
    pos_tile = tile_rows(held_pos, 256)

    def set_values(start, count, values):
        for head in range(HEADS):
            vaug[head, pl.ds(start, count), :inner] = jnp.where(
                lane_head == head, values, 0.0
            ).astype(jnp.bfloat16)

    def scaled(values):
        return (values.astype(jnp.bfloat16).astype(jnp.float32) * scale).astype(jnp.bfloat16)

    @pl.loop(0, rows_all // mlp_tile)
    def _(step):
        rows = pl.ds(pl.multiple_of(step * mlp_tile, mlp_tile), mlp_tile)
        start = tok0_ref[rows, :]
        tok[rows, :] = start
        q1[rows, :] = scaled(bdot(start.astype(jnp.bfloat16), win_ref[0, 0]))

    swap_final.wait()
    for half in range(2):
        img[half * pos_dev : (half + 1) * pos_dev, :] = fin[half].astype(jnp.float32)

    copies = []
    for layer in range(LAYERS):

        @pl.loop(0, held_pos // pos_tile)
        def _(step):
            start = pl.multiple_of(step * pos_tile, pos_tile)
            rows = pl.ds(start, pos_tile)
            here = img[rows, :]
            key_b = (here + code_ref[rows, :]).astype(jnp.bfloat16)
            k1[rows, :] = bdot(key_b, win_ref[layer, 1]).astype(jnp.bfloat16)
            q2[rows, :] = scaled(bdot(key_b, win_ref[layer, 3]))
            values = bdot(here.astype(jnp.bfloat16), win_ref[layer, 2])
            set_values(start, pos_tile, values)

        @pl.loop(0, rows_all // tok_tile)
        def _(step):
            rows = pl.ds(pl.multiple_of(step * tok_tile, tok_tile), tok_tile)
            total, peaks = head_attend(q1[rows, :], k1, vaug, held_pos, lane_head, None)
            sums = total[:, inner:]
            part_a[layer, rows, :] = (total[:, :inner] / sums).astype(jnp.bfloat16)
            logs = jnp.log(sums)
            compact = jnp.zeros((tok_tile, inner), jnp.float32)
            for head in range(HEADS):
                column = peaks[head] + logs[:, head * head_size : head * head_size + 1]
                compact = jnp.where(lane == head, column, compact)
            lse[rows, :] = compact

        turned = jnp.transpose(lse[...])[:HEADS, :]
        for peer in range(members):
            part_l[layer, peer] = turned[:, peer * own : (peer + 1) * own]
        waits = []
        for step in range(1, members):
            peer = peer_rank(step)
            target = peer * 2 + bit
            waits.append(
                (
                    send(
                        part_a.at[layer, pl.ds(pl.multiple_of(peer * own, own), own)],
                        recv_a.at[layer, step],
                        a_send.at[layer, step],
                        a_recv.at[layer, step],
                        target,
                    ),
                    send(
                        part_l.at[layer, peer],
                        recv_l.at[layer, step],
                        l_send.at[layer, step],
                        l_recv.at[layer, step],
                        target,
                    ),
                )
            )
        own_rows = pl.ds(pl.multiple_of(rank * own, own), own)
        blocks = [part_a[layer, own_rows, :]]
        marks = [part_l[layer, rank]]
        for step in range(1, members):
            waits[step - 1][0].wait_recv()
            waits[step - 1][1].wait_recv()
            blocks.append(recv_a[layer, step])
            marks.append(recv_l[layer, step])
        highest = functools.reduce(jnp.maximum, marks)
        shares = [jnp.exp(mark - highest) for mark in marks]
        whole = functools.reduce(jnp.add, shares)
        spread = jnp.where(
            lax.broadcasted_iota(jnp.int32, (HEADS, inner), 1) // head_size
            == lax.broadcasted_iota(jnp.int32, (HEADS, inner), 0),
            1.0,
            0.0,
        )
        mixed = None
        for block, share in zip(blocks, shares):
            factor = lax.dot_general(
                share / whole,
                spread,
                (((0,), (0,)), ((), ())),
                preferred_element_type=jnp.float32,
                precision=lax.Precision.HIGHEST,
            )
            term = factor * block.astype(jnp.float32)
            mixed = term if mixed is None else mixed + term
        a1_all[layer, own_rows, :] = mixed.astype(jnp.bfloat16)
        shared = []
        for step in range(1, members):
            shared.append(
                send(
                    a1_all.at[layer, own_rows],
                    a1_all.at[layer, own_rows],
                    g_send.at[layer, step],
                    g_recv.at[layer, step],
                    peer_rank(step) * 2 + bit,
                )
            )
        for pair in waits:
            pair[0].wait_send()
            pair[1].wait_send()
        for copy in shared:
            copy.wait()

        @pl.loop(0, rows_all // mlp_tile)
        def _(step):
            start = pl.multiple_of(step * mlp_tile, mlp_tile)
            rows = pl.ds(start, mlp_tile)
            two = norm_rows(tok[rows, :] + bdot(a1_all[layer, rows, :], wout_ref[layer, 0]))
            hidden = jax.nn.relu(bdot(two.astype(jnp.bfloat16), up_ref[layer])).astype(jnp.bfloat16)
            three = norm_rows(two + bdot(hidden, down_ref[layer]))
            tok[rows, :] = three
            three_b = three.astype(jnp.bfloat16)
            k2[rows, :] = bdot(three_b, win_ref[layer, 4]).astype(jnp.bfloat16)
            set_values(start, mlp_tile, bdot(three_b, win_ref[layer, 5]))
            if layer < LAYERS - 1:
                q1[rows, :] = scaled(bdot(three_b, win_ref[layer + 1, 0]))
            else:
                tok3b[rows, :] = three_b

        @pl.loop(0, held_pos // pos_tile)
        def _(step):
            rows = pl.ds(pl.multiple_of(step * pos_tile, pos_tile), pos_tile)
            total, _ = head_attend(q2[rows, :], k2, vaug, rows_all, lane_head, bias_ref[...])
            second = (total[:, :inner] / total[:, inner:]).astype(jnp.bfloat16)
            img[rows, :] = norm_rows(img[rows, :] + bdot(second, wout_ref[layer, 1]))

    swap_hq.wait()
    prompts = out_ref.shape[0]
    pick = jnp.where(
        lax.broadcasted_iota(jnp.int32, (prompts, rows_all), 1)
        == lax.broadcasted_iota(jnp.int32, (prompts, rows_all), 0) * TOKS_P + (TOKS_P - 3),
        1.0,
        0.0,
    ).astype(jnp.bfloat16)
    slots = bdot(pick, tok3b[...]).astype(jnp.bfloat16)
    hyper = bdot(slots, whyper_ref[...]).astype(jnp.bfloat16)
    for half in range(2):
        span = slice(half * pos_dev, (half + 1) * pos_dev)
        feats = (img[span, :] + hqs[half].astype(jnp.float32)).astype(jnp.bfloat16)
        logits = lax.dot_general(
            hyper, feats, (((1,), (1,)), ((), ())), preferred_element_type=jnp.float32
        ) * width ** (-0.5)
        out_ref[:, half, :] = jnp.where(live_ref[...] > 0.0, logits, 0.0).astype(jnp.bfloat16)


def run_decode(members, final, hq, code, tok0, bias, live, win, wout, up, down, whyper):
    pos_dev, width = final.shape[1:]
    held_pos = 2 * pos_dev
    rows_all = tok0.shape[0]
    own = rows_all // members
    inner = win.shape[-1]
    prompts = live.shape[0]
    f32, bf16 = jnp.float32, jnp.bfloat16
    vmem = pltpu.VMEM
    dma = pltpu.SemaphoreType.DMA
    return pl.pallas_call(
        functools.partial(decode_kernel, members),
        out_shape=jax.ShapeDtypeStruct((prompts, 2, pos_dev), bf16),
        in_specs=[pl.BlockSpec(memory_space=vmem)] * 11,
        out_specs=pl.BlockSpec(memory_space=vmem),
        scratch_shapes=[
            vmem((2, pos_dev, width), bf16),
            vmem((2, pos_dev, width), bf16),
            vmem((held_pos, width), f32),
            vmem((rows_all, width), f32),
            vmem((rows_all, width), bf16),
            vmem((HEADS, max(held_pos, rows_all), 2 * inner), bf16),
            vmem((rows_all, inner), bf16),
            vmem((held_pos, inner), bf16),
            vmem((held_pos, inner), bf16),
            vmem((rows_all, inner), bf16),
            vmem((LAYERS, rows_all, inner), bf16),
            vmem((LAYERS, members, HEADS, own), f32),
            vmem((rows_all, inner), f32),
            vmem((LAYERS, members, own, inner), bf16),
            vmem((LAYERS, members, HEADS, own), f32),
            vmem((LAYERS, rows_all, inner), bf16),
            dma((2,)),
            dma((2,)),
        ]
        + [dma((LAYERS, members))] * 6,
        compiler_params=pltpu.CompilerParams(
            collective_id=0, has_side_effects=True, vmem_limit_bytes=60 * 2**20
        ),
    )(final, hq, code, tok0, bias, live, win, wout, up, down, whyper)


def shards(
    early_feats,
    final_embed,
    prompt_counts,
    box_pixels,
    pair_table,
    token_table,
    pe_basis,
    w_early,
    attend_in,
    attend_out,
    mlp_up,
    mlp_down,
    w_hyper,
):
    images = early_feats.shape[0]
    pos_dev = early_feats.shape[1]
    prompts = box_pixels.shape[1]
    devices = lax.axis_size("img")
    my_index = lax.axis_index("img")
    my_section = lax.axis_index("section")
    members = devices // images
    my_bit = my_index % images
    first_pos = (my_index // images) * images * pos_dev
    mine = my_section * images + my_bit
    count = lax.dynamic_index_in_dim(prompt_counts, mine, 0, keepdims=False)
    boxes = lax.dynamic_index_in_dim(box_pixels, mine, 0, keepdims=False)
    hq = make_hq(early_feats, w_early)
    tok0 = start_tokens(boxes, token_table, pe_basis)
    code = grid_code(first_pos, images * pos_dev, pe_basis)
    slots = jnp.arange(prompts * TOKS_P, dtype=jnp.int32)[None, :] // TOKS_P
    bias = jnp.where(slots < count, 0.0, -jnp.inf).astype(jnp.float32)
    live = (jnp.arange(prompts, dtype=jnp.int32)[:, None] < count).astype(jnp.float32)
    masks = run_decode(
        members,
        final_embed,
        hq,
        code,
        tok0,
        bias,
        live,
        attend_in,
        attend_out,
        mlp_up,
        mlp_down,
        w_hyper,
    )
    keep = lax.dynamic_index_in_dim(masks, my_bit, 1, keepdims=False)
    sent = lax.dynamic_index_in_dim(masks, 1 - my_bit, 1, keepdims=False)
    got = lax.ppermute(sent, "img", [(i, i ^ 1) for i in range(devices)])
    result = jnp.stack([jnp.where(my_bit == 0, keep, got), jnp.where(my_bit == 0, got, keep)])
    gathered = lax.all_gather(result, "section", axis=0, tiled=True)
    outputs = lax.dynamic_slice_in_dim(pair_table, my_section * images, images, 0)
    return jnp.concatenate(
        [
            lax.dynamic_slice_in_dim(gathered, outputs[i], 1, 0).astype(jnp.float32)
            for i in range(images)
        ]
    )


def solution(mesh):
    placed = (
        P("section", "img", None),
        P("section", "img", None),
        P(),
        P(),
        P(),
        P(),
        P(),
        P(),
        P(),
        P(),
        P(),
        P(),
        P(),
    )
    return jax.shard_map(
        shards, mesh=mesh, in_specs=placed, out_specs=P("section", None, "img"), check_vma=False
    )
```
